32 devices in a mesh: member: 8 (over z, y), band: 4 (over x, core).
Axes of the slice: x: 2, y: 2, z: 4, core: 2. Of those that a mesh axis runs over, the one named last changes fastest.
Arguments:
- spectral: float32 [128, 768, 768], P('member', 'band'), parts along dimension 0, may hold values from -6 to 6
- coupling: float32 [8192, 1024], P(('member', 'band')), parts along dimension 0, may hold values from 0.02 to 162, as said below
- quadratic: float32 [8192, 1024], P(('member', 'band')), parts along dimension 0, may hold values from -1.5 to 1.5
Outputs:
- tendency_spectral: float32 [128, 768, 768], P('member', 'band'), parts along dimension 0
The draws below stay inside these ranges and needn't reach their ends.
There are 8 independent parts, one for each index of `member`. The reference program is written for one: setup_inputs(seed, part) draws one part's arguments, and reference() takes and returns one part's arrays. A program takes and returns all parts, laid end to end along the dimension named above; each array names one. Nothing has to cross between parts.
Inputs may be any that keep to these rules, and one draw needn't show every extreme that they name: `coupling`: positive.
All inputs are finite; a program needn't handle non-finite values.
Results may differ from the reference program's by a relative error of at most 0.00008.
Values sent between devices are 32-bit elements; how exact they have to be, the bound alone decides.
A program may use at most 128 MiB of HBM per device.

```python
import math
import jax
import jax.numpy as jnp
from jax import lax

N = 1024
LEVELS = 16
KS = 768


def draw_coupling(key, part):
    keys = jax.random.split(jax.random.fold_in(key, 11), 3)
    rows = jnp.arange(N, dtype=jnp.float32) / N
    row_noise = jax.random.uniform(keys[0], (N,), jnp.float32)
    col_noise = jax.random.uniform(keys[1], (N,), jnp.float32)
    trend = jnp.exp(jnp.log(3.0) * rows)
    cell = jax.random.uniform(keys[2], (N, N), jnp.float32, 0.5, 1.5)
    row_scale = trend * jnp.exp(jnp.log(10.0) * row_noise)
    col_scale = jnp.exp(jnp.log(10.0) * col_noise)
    return (row_scale[:, None] * col_scale[None, :] * cell / 10.0).astype(jnp.float32)


def block_levels(stream_key, extent, shards, smallest, largest):
    def one(dim, shards_of):
        steps = jax.random.uniform(jax.random.fold_in(jax.random.fold_in(stream_key, 6), dim), (shards_of,), jnp.float32, smallest / len(shards), largest / len(shards))
        return jnp.repeat(jnp.exp(steps), extent[dim] // shards_of).reshape((-1,) + (1,) * (len(extent) - dim - 1))

    gain = one(*shards[0])
    for cut in shards[1:]:
        gain = gain * one(*cut)
    return gain


def noise(stream_key, shape, deviation, most, cuts=(), kind=jnp.bfloat16):
    result = deviation * jax.random.normal(stream_key, shape, jnp.float32)
    if cuts:
        result = result * block_levels(stream_key, shape, cuts, -0.22, 0.18)
    return jnp.clip(result, -most, most).astype(kind)


def setup_inputs(seed: int = 0, part: int = 0) -> dict:
    seeds = jax.random.split(jax.random.key(seed), 4)
    part_splits = jax.random.split(jax.random.fold_in(seeds[3], part), 4)
    spectral = noise(part_splits[0], (LEVELS, KS, KS), 1.0, 6.0, ((1, 4),), jnp.float32)
    coupling = draw_coupling(jax.random.fold_in(jax.random.fold_in(seeds[3], part), 71), part)
    quadratic = noise(part_splits[2], (N, N), 0.25, 1.5, ((0, 4),), jnp.float32)
    return {"spectral": spectral, "coupling": coupling, "quadratic": quadratic}


def tables(cells, coeffs):
    half_count = coeffs // 2
    position = jnp.arange(cells, dtype=jnp.int32)
    column = jnp.arange(coeffs, dtype=jnp.int32)
    wavenumber = jnp.where(column < half_count, column, column - half_count)
    turns = position[:, None] * wavenumber[None, :] % cells
    angles = turns.astype(jnp.float32) * (2.0 * math.pi / cells)
    basis_table = jnp.where(column[None, :] < half_count, jnp.cos(angles), jnp.sin(angles))
    synthesis = basis_table / math.sqrt(half_count)
    factor = jnp.where(wavenumber == 0, 1.0, 2.0) * (math.sqrt(half_count) / cells)
    analysis = (basis_table * factor[None, :]).T
    return (synthesis, analysis)

def reference(spectral, coupling, quadratic):
    synthesis, analysis = tables(N, KS)
    high = lax.Precision.HIGHEST
    section = jnp.einsum('lab,yb->lay', spectral, synthesis, precision=high)
    grid = jnp.einsum('xa,lay->lyx', synthesis, section, precision=high)
    product = coupling[None] * grid
    energy = lax.optimization_barrier(jnp.mean(product * product, axis=(1, 2)))
    scaled = product / jnp.sqrt(energy + 1e-06)[:, None, None]
    tendency = scaled + quadratic[None] * scaled * scaled
    back = jnp.einsum('ax,lyx->lya', analysis, tendency, precision=high)
    return jnp.einsum('by,lya->lab', analysis, back, precision=high)
```

```python
import math

import jax
import jax.numpy as jnp
from jax import lax
from jax.sharding import PartitionSpec as P


def tables(cells, coeffs):
    half_count = coeffs // 2
    position = jnp.arange(cells, dtype=jnp.int32)
    column = jnp.arange(coeffs, dtype=jnp.int32)
    wavenumber = jnp.where(column < half_count, column, column - half_count)
    turns = position[:, None] * wavenumber[None, :] % cells
    angles = turns.astype(jnp.float32) * (2.0 * math.pi / cells)
    basis_table = jnp.where(column[None, :] < half_count, jnp.cos(angles), jnp.sin(angles))
    synthesis = basis_table / math.sqrt(half_count)
    factor = jnp.where(wavenumber == 0, 1.0, 2.0) * (math.sqrt(half_count) / cells)
    analysis = (basis_table * factor[None, :]).T
    return (synthesis, analysis)


def on_device(spectral, coupling, quadratic):
    high = lax.Precision.HIGH
    levels, band, coeffs = spectral.shape
    cells = coupling.shape[1]
    ways = lax.axis_size("band")
    synthesis, analysis = tables(cells, coeffs)
    points = float(cells * cells)

    arrived = [
        lax.all_to_all(spectral[at : at + ways], "band", split_axis=0, concat_axis=0, tiled=True)
        for at in range(0, levels, ways)
    ]
    coupling = lax.all_gather(coupling, "band", axis=0, tiled=True)
    quadratic = lax.all_gather(quadratic, "band", axis=0, tiled=True)
    outputs = []
    for field in arrived:
        field = field.reshape(coeffs, coeffs)
        section = jnp.einsum("xa,ab->xb", synthesis, field, precision=high)
        grid = jnp.einsum("yb,xb->yx", synthesis, section, precision=high)
        product = coupling * grid
        energy = jnp.sum(product * product) / points
        scaled = product * (1.0 / jnp.sqrt(energy + 1e-06))
        tendency = scaled + quadratic * scaled * scaled
        back = jnp.einsum("ax,yx->ay", analysis, tendency, precision=high)
        done = jnp.einsum("ay,by->ab", back, analysis, precision=high)
        done = done.reshape(ways, band, coeffs)
        outputs.append(lax.all_to_all(done, "band", split_axis=0, concat_axis=0, tiled=True))
    return jnp.concatenate(outputs, axis=0)


def solution(mesh):
    placed = (P("member", "band", None), P(("member", "band"), None), P(("member", "band"), None))
    return jax.shard_map(
        on_device, mesh=mesh, in_specs=placed, out_specs=P("member", "band", None), check_vma=False
    )
```
